32 devices in a mesh: seq: 8 (over y, x, core), heads: 4 (over z).
Axes of the slice: x: 2, y: 2, z: 4, core: 2. Of those that a mesh axis runs over, the one named last changes fastest.
Arguments:
- queries: bfloat16 [2048, 16, 128], P('seq', 'heads'), may hold values from -6 to 6
- key_vecs: bfloat16 [2048, 16, 128], P('seq', 'heads'), may hold values from -12 to 12
- values: bfloat16 [2048, 32, 128], P('seq', 'heads'), may hold values from -6 to 6
- strength: float32 [2048, 32], P('seq', 'heads'), may hold values from 0 to 1, as said below
- decay_rate: float32 [2048, 32], P('seq', 'heads'), may hold values from 0 to 0.15, as said below
- norm_gain: float32 [128], replicated, may hold values from 0.5 to 1.5
- w_out: bfloat16 [4096, 2048], P('heads'), may hold values from -0.09375 to 0.09375
Outputs:
- mixed: bfloat16 [2048, 2048], P(('seq', 'heads'))
The draws below stay inside these ranges and needn't reach their ends.
Inputs may be any that keep to these rules, and one draw needn't show every extreme that they name: Every write strength lies strictly between 0 and 1. `decay_rate`: every decay rate is positive.
All inputs are finite; a program needn't handle non-finite values.
Results may differ from the reference program's by a relative error of at most 0.0049.
Values sent between devices are 32-bit elements; how exact they have to be, the bound alone decides.
A program may use at most 192 MiB of HBM per device.

```python
import math
import jax
import jax.numpy as jnp
from jax import lax

D = 2048
DK = 128
DV = 128
HQK = 16
VALUE_HEADS = 32
BLOCK_TOKENS = 64
TOK_DEV = 256
SEQUENCE_TOKENS = 2048


def head_classes(key):
    head_order = jax.random.permutation(jax.random.fold_in(key, 11), VALUE_HEADS)
    fast_count = VALUE_HEADS // 2
    return head_order < fast_count


def logarithmic_uniform_draw(key, shape, low, high):
    return jnp.exp(jax.random.uniform(key, shape, jnp.float32, math.log(low), math.log(high)))


def draw_key_vecs(key, part):
    device_random_keys = jax.random.split(jax.random.fold_in(key, 41), 4)
    total_block_count = SEQUENCE_TOKENS // BLOCK_TOKENS
    base_noise = jnp.clip(jax.random.normal(device_random_keys[0], (SEQUENCE_TOKENS, HQK, DK), jnp.float32), -6.0, 6.0)
    shared = jnp.clip(jax.random.normal(device_random_keys[1], (HQK, DK), jnp.float32), -4.0, 4.0)
    block_signs = jnp.where(jax.random.bernoulli(device_random_keys[2], 0.5, (total_block_count, HQK)), 1.0, -1.0)
    block_weights = jax.random.uniform(device_random_keys[3], (total_block_count, HQK), jnp.float32, 0.8, 1.2)
    per_block = jnp.repeat(block_signs * block_weights, BLOCK_TOKENS, axis=0)
    return (base_noise + per_block[:, :, None] * shared[None, :, :]).astype(jnp.bfloat16)


def draw_strength(key, part):
    fast_heads = head_classes(key)
    device_random_keys = jax.random.split(jax.random.fold_in(key, 23), 6)
    total_block_count = SEQUENCE_TOKENS // BLOCK_TOKENS
    sudden_head_fraction = min(8.0 * BLOCK_TOKENS / SEQUENCE_TOKENS, 0.25)
    fast_level = logarithmic_uniform_draw(device_random_keys[0], (VALUE_HEADS,), 0.3, 0.9)
    gentle_decay_level = logarithmic_uniform_draw(device_random_keys[1], (VALUE_HEADS,), 0.1, 0.5) * (DK / SEQUENCE_TOKENS)
    rough_fast = jax.random.uniform(device_random_keys[2], (SEQUENCE_TOKENS, VALUE_HEADS), jnp.float32, 0.6, 1.1)
    noisy_gentle_decay = logarithmic_uniform_draw(device_random_keys[3], (SEQUENCE_TOKENS, VALUE_HEADS), 0.5, 2.0)
    sudden_decay_blocks = jax.random.bernoulli(device_random_keys[4], sudden_head_fraction, (total_block_count, VALUE_HEADS))
    sudden_decay_values = logarithmic_uniform_draw(device_random_keys[5], (SEQUENCE_TOKENS, VALUE_HEADS), 0.025, 0.048)
    sudden_decay_full = jnp.repeat(sudden_decay_blocks, BLOCK_TOKENS, axis=0)
    fast_vals = fast_level[None, :] * rough_fast
    gentle_decay_values = jnp.where(sudden_decay_full, sudden_decay_values, gentle_decay_level[None, :] * noisy_gentle_decay)
    return jnp.where(fast_heads[None, :], fast_vals, gentle_decay_values).astype(jnp.float32)


def draw_decay_rate(key, part):
    fast_heads = head_classes(key)
    device_random_keys = jax.random.split(jax.random.fold_in(key, 31), 4)
    fast_level = logarithmic_uniform_draw(device_random_keys[0], (VALUE_HEADS,), min(1.0 / TOK_DEV, 1.0 / 80.0), 1.0 / 40.0)
    gentle_decay_level = logarithmic_uniform_draw(device_random_keys[1], (VALUE_HEADS,), 0.1, 0.5) / SEQUENCE_TOKENS
    rough = logarithmic_uniform_draw(device_random_keys[2], (SEQUENCE_TOKENS, VALUE_HEADS), 0.5, 2.0)
    segment = logarithmic_uniform_draw(device_random_keys[3], (SEQUENCE_TOKENS // TOK_DEV, VALUE_HEADS), 0.5, 2.0)
    segment_full = jnp.repeat(segment, TOK_DEV, axis=0)
    head_level = jnp.where(fast_heads, fast_level, gentle_decay_level)
    return (head_level[None, :] * rough * segment_full).astype(jnp.float32)


def levels(stream_key, extent, cuts, smallest, largest):
    def one(axis_at, shards_of):
        draws = jax.random.uniform(jax.random.fold_in(jax.random.fold_in(stream_key, 6), axis_at), (shards_of,), jnp.float32, smallest / len(cuts), largest / len(cuts))
        return jnp.repeat(jnp.exp(draws), extent[axis_at] // shards_of).reshape((-1,) + (1,) * (len(extent) - axis_at - 1))

    loudness = one(*cuts[0])
    for cut in cuts[1:]:
        loudness = loudness * one(*cut)
    return loudness


def noise(rng, dims, width, bound, shards=(), kind=jnp.bfloat16):
    drawn = width * jax.random.normal(rng, dims, jnp.float32)
    if shards:
        drawn = drawn * levels(rng, dims, shards, -0.22, 0.18)
    return jnp.clip(drawn, -bound, bound).astype(kind)


def setup_inputs(seed: int = 0) -> dict:
    splits = jax.random.split(jax.random.key(seed), 8)
    return {
        "queries": noise(splits[0], (SEQUENCE_TOKENS, HQK, DK), 1.0, 6.0, ((0, 8), (1, 4))),
        "key_vecs": draw_key_vecs(jax.random.fold_in(splits[7], 71), 0),
        "values": noise(splits[2], (SEQUENCE_TOKENS, VALUE_HEADS, DV), 1.0, 6.0, ((0, 8), (1, 4))),
        "strength": draw_strength(jax.random.fold_in(splits[7], 71), 0),
        "decay_rate": draw_decay_rate(jax.random.fold_in(splits[7], 71), 0),
        "norm_gain": jnp.clip(1.0 + 0.1 * jax.random.normal(splits[5], (DV,), jnp.float32), 0.5, 1.5),
        "w_out": noise(splits[6], (VALUE_HEADS * DV, D), (VALUE_HEADS * DV) ** -0.5, 0.09375, ((0, 4),)),
    }


strict_precision = lax.Precision.HIGHEST
norm_eps = 1e-12
unit_eps = 1e-06

def unit_rows(matrix):
    matrix = matrix.astype(jnp.float32)
    return matrix / jnp.sqrt(lax.optimization_barrier(jnp.sum(matrix * matrix, axis=-1, keepdims=True)) + unit_eps)

def prepare(query_blk, key_blk, value_blk, strength_blk, decay_blk):
    group_size = value_blk.shape[1] // query_blk.shape[1]
    normalized_queries = jnp.repeat(jnp.transpose(unit_rows(query_blk), (1, 0, 2)), group_size, axis=0)
    keys_n = jnp.repeat(jnp.transpose(unit_rows(key_blk), (1, 0, 2)), group_size, axis=0)
    values_f = jnp.transpose(value_blk.astype(jnp.float32), (1, 0, 2))
    writes = jnp.transpose(strength_blk)
    decay_logarithm = -jnp.cumsum(jnp.transpose(decay_blk), axis=1)
    return (normalized_queries, keys_n, values_f, writes, decay_logarithm)

def block_parts(normalized_queries, keys_n, values_f, writes, decay_logarithm):
    key_width = keys_n.shape[2]
    length = keys_n.shape[1]
    row_ids = lax.broadcasted_iota(jnp.int32, (length, length), 0)
    col_ids = lax.broadcasted_iota(jnp.int32, (length, length), 1)
    ratios = jnp.exp(jnp.minimum(decay_logarithm[:, :, None] - decay_logarithm[:, None, :], 0.0))
    key_dots = jnp.einsum('hik,hjk->hij', keys_n, keys_n, precision=strict_precision)
    query_dots = jnp.einsum('hik,hjk->hij', normalized_queries, keys_n, precision=strict_precision)
    system = jnp.where(row_ids > col_ids, writes[:, :, None] * ratios * key_dots, 0.0)
    system = system + jnp.eye(length, dtype=jnp.float32)
    scaled = writes * jnp.exp(decay_logarithm)
    right_side = jnp.concatenate([scaled[:, :, None] * keys_n, writes[:, :, None] * values_f], axis=2)
    solved = jax.scipy.linalg.solve_triangular(system, right_side, lower=True, unit_diagonal=True)
    weighted_key_rows = solved[:, :, :key_width]
    corrected_values = solved[:, :, key_width:]
    mixing = jnp.where(row_ids >= col_ids, ratios * query_dots, 0.0)
    trailing_keys = jnp.exp(decay_logarithm[:, -1:] - decay_logarithm)[:, :, None] * keys_n
    return (weighted_key_rows, corrected_values, mixing, trailing_keys)

def block_apply(memory_state, normalized_queries, decay_logarithm, weighted_key_rows, corrected_values, mixing, trailing_keys):
    state_increment = corrected_values - jnp.einsum('qjl,qlo->qjo', weighted_key_rows, memory_state, precision=strict_precision)
    output_rows = jnp.exp(decay_logarithm)[:, :, None] * jnp.einsum('qjl,qlo->qjo', normalized_queries, memory_state, precision=strict_precision)
    output_rows = output_rows + jnp.einsum('hij,hjv->hiv', mixing, state_increment, precision=strict_precision)
    updated_state = jnp.exp(decay_logarithm[:, -1])[:, None, None] * memory_state
    updated_state = updated_state + jnp.einsum('oqm,oqy->omy', trailing_keys, state_increment, precision=strict_precision)
    return (updated_state, output_rows)

def normalize(output_rows, norm_gain):
    mean_sq = lax.optimization_barrier(jnp.mean(output_rows * output_rows, axis=-1, keepdims=True))
    return (output_rows / jnp.sqrt(mean_sq + norm_eps) * norm_gain).astype(jnp.bfloat16)

def reference(queries, key_vecs, values, strength, decay_rate, norm_gain, w_out):
    total_len = queries.shape[0]
    block_count = total_len // BLOCK_TOKENS
    heads_v = values.shape[1]
    blocks = (queries.reshape(block_count, BLOCK_TOKENS, HQK, DK), key_vecs.reshape(block_count, BLOCK_TOKENS, HQK, DK), values.reshape(block_count, BLOCK_TOKENS, heads_v, DV), strength.reshape(block_count, BLOCK_TOKENS, heads_v), decay_rate.reshape(block_count, BLOCK_TOKENS, heads_v))

    def advance(memory_state, pieces):
        prepared = prepare(pieces[0], pieces[1], pieces[2], pieces[3], pieces[4])
        weighted_key_rows, corrected_values, mixing, trailing_keys = block_parts(*prepared)
        updated_state, output_rows = block_apply(memory_state, prepared[0], prepared[4], weighted_key_rows, corrected_values, mixing, trailing_keys)
        return (updated_state, normalize(jnp.transpose(output_rows, (1, 0, 2)), norm_gain))
    start_state = jnp.zeros((heads_v, DK, DV), jnp.float32)
    _, normed = lax.scan(advance, start_state, blocks)
    flat = normed.reshape(total_len, heads_v * DV)
    mixed = jnp.dot(flat.astype(jnp.float32), w_out.astype(jnp.float32), precision=strict_precision)
    return mixed.astype(jnp.bfloat16)
```

```python
import functools

import jax
import jax.numpy as jnp
from jax import lax
from jax.experimental import pallas as pl
from jax.experimental.pallas import tpu as pltpu
from jax.sharding import PartitionSpec as P

norm_eps = 1e-12
unit_eps = 1e-06
BASE = 16
HALF = 128
f32, bf16 = jnp.float32, jnp.bfloat16

NN = (((1,), (0,)), ((), ()))
NT = (((1,), (1,)), ((), ()))
TN = (((0,), (0,)), ((), ()))


def mm(a, b, dims=NN):
    return lax.dot_general(a, b, dims, preferred_element_type=f32)


def split(x):
    high = x.astype(bf16)
    return high, (x - high.astype(f32)).astype(bf16)


def split3(x):
    high = x.astype(bf16)
    rest = x - high.astype(f32)
    mid = rest.astype(bf16)
    return high, mid, (rest - mid.astype(f32)).astype(bf16)


def mm3(a, b, dims=NN):
    return mm(a[0], b[0], dims) + (mm(a[0], b[1], dims) + mm(a[1], b[0], dims))


def iota(shape, dim):
    return lax.broadcasted_iota(jnp.int32, shape, dim)


def diagonal_inverses(systems, length):
    count = length // BASE
    lane = iota((BASE, length), 1)
    packed = []
    for low in systems:
        rows = jnp.zeros((BASE, length), f32)
        for b in range(count):
            rows = rows + jnp.where(lane // BASE == b, low[b * BASE : (b + 1) * BASE], 0.0)
        packed.append(rows)
    packed = jnp.concatenate(packed, axis=0)
    total = packed.shape[0]
    parts = []
    for start in range(0, length, 128):
        chunk = packed[:, start : start + 128]
        group = iota((total, 128), 1) // BASE * BASE
        local = iota((total, 128), 1) % BASE
        parts.append((chunk, group))
    outs = []
    for chunk, group in parts:
        solved = [
            jnp.where(iota((BASE, 128), 0) == iota((BASE, 128), 1) % BASE, 1.0, 0.0).astype(f32)
            for _ in systems
        ]
        for j in range(BASE - 1):
            column = jnp.take_along_axis(chunk, group + j, axis=1)
            solved = [
                x - column[n * BASE : (n + 1) * BASE] * x[j : j + 1] for n, x in enumerate(solved)
            ]
        outs.append(solved)
    return [[outs[c][n] for c in range(len(outs))] for n in range(len(systems))]


def spread(block):
    lane = iota((BASE, HALF), 1)
    return jnp.concatenate(
        [jnp.where(lane // BASE == b, block, 0.0) for b in range(HALF // BASE)], axis=0
    )


def local_kernel(
    group_size, q_ref, k_ref, v_ref, strength_ref, decay_ref, transit_ref, offset_ref, reach_ref, near_ref
):
    step = pl.program_id(0)
    length = q_ref.shape[0]
    heads = decay_ref.shape[1]
    width = k_ref.shape[1]
    query, key = q_ref[...], k_ref[...]
    query_f, key_f = query.astype(f32), key.astype(f32)
    query_scale = lax.rsqrt(jnp.sum(query_f * query_f, axis=1, keepdims=True) + unit_eps)
    key_sq = key_f * key_f
    key_scale = lax.rsqrt(jnp.sum(key_sq, axis=1, keepdims=True) + unit_eps)
    ones = jnp.ones((8, width), bf16)
    sq_high, sq_low = split(key_sq)
    key_scale_row = lax.rsqrt(mm(ones, sq_high, NT)[:1] + mm(ones, sq_low, NT)[:1] + unit_eps)

    row, col = iota((length, length), 0), iota((length, length), 1)
    lower = jnp.where(row >= col, 1.0, 0.0).astype(bf16)
    upper = jnp.where(row <= col, 1.0, 0.0).astype(bf16)
    pieces = split3(-decay_ref[...])
    logs = mm(lower, pieces[0]) + (mm(lower, pieces[1]) + mm(lower, pieces[2]))
    logs_row = mm(pieces[0], upper, TN) + (mm(pieces[1], upper, TN) + mm(pieces[2], upper, TN))

    key_dots = mm(key, key, NT) * key_scale * key_scale_row
    query_dots = mm(query, key, NT) * query_scale * key_scale_row

    half = [slice(s, s + HALF) for s in range(0, length, HALF)]
    systems, mixings, log_cols, writes = [], [], [], []
    for n in range(group_size):
        head = step * group_size + n
        lane = iota((length, heads), 1)
        log_col = jnp.sum(jnp.where(lane == head, logs, 0.0), axis=1, keepdims=True)
        write = jnp.sum(jnp.where(lane == head, strength_ref[...], 0.0), axis=1, keepdims=True)
        log_row = jnp.sum(
            jnp.where(iota((heads, length), 0) == head, logs_row, 0.0), axis=0, keepdims=True
        )
        ratio = jnp.exp(jnp.minimum(log_col - log_row, 0.0))
        systems.append(jnp.where(row > col, write * ratio * key_dots, 0.0))
        mixings.append(jnp.where(row >= col, ratio * query_dots, 0.0))
        log_cols.append(log_col)
        writes.append(write)

    base = diagonal_inverses(systems, length)
    r, c = iota((HALF, HALF), 0), iota((HALF, HALF), 1)
    units = [(n, s) for n in range(group_size) for s in range(len(half))]
    inverse = {u: spread(base[u[0]][u[1]]) for u in units}
    size = BASE
    while size < HALF:
        joint = (r // (2 * size) == c // (2 * size)) & (r // size > c // size)
        halves = {u: split(inverse[u]) for u in units}
        between = {
            u: mm3(split(jnp.where(joint, systems[u[0]][half[u[1]], half[u[1]]], 0.0)), halves[u])
            for u in units
        }
        inverse = {u: inverse[u] - mm3(halves[u], split(between[u])) for u in units}
        size *= 2
    inverse = {u: split(inverse[u]) for u in units}

    solved = [[] for _ in range(group_size)]
    for s in range(len(half)):
        for n in range(group_size):
            write = writes[n][half[s]]
            key_part = (write * jnp.exp(log_cols[n][half[s]]) * key_scale[half[s]]) * key_f[half[s]]
            value_part = write * v_ref[half[s], n * width : (n + 1) * width].astype(f32)
            right = jnp.concatenate([key_part, value_part], axis=1)
            if s:
                done = split(jnp.concatenate(solved[n], axis=0))
                right = right - mm3(split(systems[n][half[s], : s * HALF]), done)
            solved[n].append(mm3(inverse[n, s], split(right)))

    eye = jnp.where(r == c, 1.0, 0.0)
    for n in range(group_size):
        full = split(jnp.concatenate(solved[n], axis=0))
        log_col = log_cols[n]
        mixed = mm3(split(mixings[n]), full)
        reach = (jnp.exp(log_col) * query_scale) * query_f - mixed[:, :width]
        reach_ref[n] = reach
        near_ref[n] = mixed[:, width:]
        last = log_col[length - 1 :]
        trailing = split((jnp.exp(last - log_col) * key_scale) * key_f)
        maps = mm3(trailing, full, TN)
        transit_ref[n] = jnp.exp(last) * eye - maps[:, :width]
        offset_ref[n] = maps[:, width:]


def local_phase(queries, key_vecs, values, strength, decay_rate, interpret=False):
    length, heads_k, width = queries.shape
    heads_v = values.shape[1]
    group_size = heads_v // heads_k
    per_head = lambda rows: pl.BlockSpec((group_size, rows, width), lambda i: (i, 0, 0))
    lanes = lambda n: pl.BlockSpec((length, n * width), lambda i: (0, i))
    whole = pl.BlockSpec((length, heads_v), lambda i: (0, 0))
    return pl.pallas_call(
        functools.partial(local_kernel, group_size),
        grid=(heads_k,),
        in_specs=[lanes(1), lanes(1), lanes(group_size), whole, whole],
        out_specs=[per_head(width), per_head(width), per_head(length), per_head(length)],
        out_shape=[
            jax.ShapeDtypeStruct((heads_v, width, width), f32),
            jax.ShapeDtypeStruct((heads_v, width, width), f32),
            jax.ShapeDtypeStruct((heads_v, length, width), f32),
            jax.ShapeDtypeStruct((heads_v, length, width), f32),
        ],
        interpret=interpret,
        name="local_phase",
    )(
        queries.reshape(length, heads_k * width),
        key_vecs.reshape(length, heads_k * width),
        values.reshape(length, heads_v * width),
        strength,
        decay_rate,
    )


def batched3(a, b):
    one = lambda x, y: jnp.einsum("hik,hkj->hij", x, y, preferred_element_type=f32)
    a, b = split(a), split(b)
    return one(a[0], b[0]) + (one(a[0], b[1]) + one(a[1], b[0]))


def body(queries, key_vecs, values, strength, decay_rate, norm_gain, w_out):
    length = queries.shape[0]
    transit, offset, reach, near = local_phase(queries, key_vecs, values, strength, decay_rate)
    count, mine = lax.axis_size("seq"), lax.axis_index("seq")
    maps = lax.all_gather(jnp.concatenate([transit, offset], axis=2), "seq")
    width = transit.shape[1]

    def lap(position, state):
        pair = maps[position]
        longer = batched3(pair[:, :, :width], state) + pair[:, :, width:]
        return jnp.where(position < mine, longer, state)

    state = lax.fori_loop(0, count - 1, lap, jnp.zeros_like(offset))
    core = near + batched3(reach, state)
    mean_sq = jnp.mean(core * core, axis=-1, keepdims=True)
    normed = (core * lax.rsqrt(mean_sq + norm_eps) * norm_gain).astype(bf16)
    flat = jnp.transpose(normed, (1, 0, 2)).reshape(length, -1)
    mixed = lax.psum_scatter(
        jnp.dot(flat, w_out, preferred_element_type=f32), "heads", scatter_dimension=0, tiled=True
    )
    return mixed.astype(bf16)


def solution(mesh):
    return jax.shard_map(
        body,
        mesh=mesh,
        in_specs=(
            P("seq", "heads", None),
            P("seq", "heads", None),
            P("seq", "heads", None),
            P("seq", "heads"),
            P("seq", "heads"),
            P(),
            P("heads", None),
        ),
        out_specs=P(("seq", "heads"), None),
        check_vma=False,
    )
```

```python
import functools

import jax
import jax.numpy as jnp
from jax import lax
from jax.experimental import pallas as pl
from jax.experimental.pallas import tpu as pltpu
from jax.sharding import PartitionSpec as P

norm_eps = 1e-12
unit_eps = 1e-06
BASE = 16
HALF = 128
f32, bf16 = jnp.float32, jnp.bfloat16

NN = (((1,), (0,)), ((), ()))
NT = (((1,), (1,)), ((), ()))
TN = (((0,), (0,)), ((), ()))


def mm(a, b, dims=NN):
    return lax.dot_general(a, b, dims, preferred_element_type=f32)


def split(x):
    high = x.astype(bf16)
    return high, (x - high.astype(f32)).astype(bf16)


def split3(x):
    high = x.astype(bf16)
    rest = x - high.astype(f32)
    mid = rest.astype(bf16)
    return high, mid, (rest - mid.astype(f32)).astype(bf16)


def mm3(a, b, dims=NN):
    return mm(a[0], b[0], dims) + (mm(a[0], b[1], dims) + mm(a[1], b[0], dims))


def iota(shape, dim):
    return lax.broadcasted_iota(jnp.int32, shape, dim)


def diagonal_inverses(systems, length):
    count = length // BASE
    lane = iota((BASE, length), 1)
    packed = []
    for low in systems:
        rows = jnp.zeros((BASE, length), f32)
        for b in range(count):
            rows = rows + jnp.where(lane // BASE == b, low[b * BASE : (b + 1) * BASE], 0.0)
        packed.append(rows)
    packed = jnp.concatenate(packed, axis=0)
    total = packed.shape[0]
    parts = []
    for start in range(0, length, 128):
        chunk = packed[:, start : start + 128]
        group = iota((total, 128), 1) // BASE * BASE
        local = iota((total, 128), 1) % BASE
        parts.append((chunk, group))
    outs = []
    for chunk, group in parts:
        solved = [
            jnp.where(iota((BASE, 128), 0) == iota((BASE, 128), 1) % BASE, 1.0, 0.0).astype(f32)
            for _ in systems
        ]
        for j in range(BASE - 1):
            column = jnp.take_along_axis(chunk, group + j, axis=1)
            solved = [
                x - column[n * BASE : (n + 1) * BASE] * x[j : j + 1] for n, x in enumerate(solved)
            ]
        outs.append(solved)
    return [[outs[c][n] for c in range(len(outs))] for n in range(len(systems))]


def spread(block):
    lane = iota((BASE, HALF), 1)
    return jnp.concatenate(
        [jnp.where(lane // BASE == b, block, 0.0) for b in range(HALF // BASE)], axis=0
    )


def local_kernel(
    group_size, q_ref, k_ref, v_ref, strength_ref, decay_ref, transit_ref, offset_ref, reach_ref, near_ref
):
    step = pl.program_id(0)
    length = q_ref.shape[0]
    heads = decay_ref.shape[1]
    width = k_ref.shape[1]
    query, key = q_ref[...], k_ref[...]
    query_f, key_f = query.astype(f32), key.astype(f32)
    query_scale = lax.rsqrt(jnp.sum(query_f * query_f, axis=1, keepdims=True) + unit_eps)
    key_sq = key_f * key_f
    key_scale = lax.rsqrt(jnp.sum(key_sq, axis=1, keepdims=True) + unit_eps)
    ones = jnp.ones((8, width), bf16)
    sq_high, sq_low = split(key_sq)
    key_scale_row = lax.rsqrt(mm(ones, sq_high, NT)[:1] + mm(ones, sq_low, NT)[:1] + unit_eps)

    row, col = iota((length, length), 0), iota((length, length), 1)
    lower = jnp.where(row >= col, 1.0, 0.0).astype(bf16)
    upper = jnp.where(row <= col, 1.0, 0.0).astype(bf16)
    pieces = split3(-decay_ref[...])
    logs = mm(lower, pieces[0]) + (mm(lower, pieces[1]) + mm(lower, pieces[2]))
    logs_row = mm(pieces[0], upper, TN) + (mm(pieces[1], upper, TN) + mm(pieces[2], upper, TN))

    key_dots = mm(key, key, NT) * key_scale * key_scale_row
    query_dots = mm(query, key, NT) * query_scale * key_scale_row

    half = [slice(s, s + HALF) for s in range(0, length, HALF)]
    systems, mixings, log_cols, writes = [], [], [], []
    for n in range(group_size):
        head = step * group_size + n
        lane = iota((length, heads), 1)
        log_col = jnp.sum(jnp.where(lane == head, logs, 0.0), axis=1, keepdims=True)
        write = jnp.sum(jnp.where(lane == head, strength_ref[...], 0.0), axis=1, keepdims=True)
        log_row = jnp.sum(
            jnp.where(iota((heads, length), 0) == head, logs_row, 0.0), axis=0, keepdims=True
        )
        ratio = jnp.exp(jnp.minimum(log_col - log_row, 0.0))
        systems.append(jnp.where(row > col, write * ratio * key_dots, 0.0))
        mixings.append(jnp.where(row >= col, ratio * query_dots, 0.0))
        log_cols.append(log_col)
        writes.append(write)

    base = diagonal_inverses(systems, length)
    r, c = iota((HALF, HALF), 0), iota((HALF, HALF), 1)
    units = [(n, s) for n in range(group_size) for s in range(len(half))]
    inverse = {u: spread(base[u[0]][u[1]]) for u in units}
    size = BASE
    while size < HALF:
        joint = (r // (2 * size) == c // (2 * size)) & (r // size > c // size)
        halves = {u: split(inverse[u]) for u in units}
        between = {
            u: mm3(split(jnp.where(joint, systems[u[0]][half[u[1]], half[u[1]]], 0.0)), halves[u])
            for u in units
        }
        inverse = {u: inverse[u] - mm3(halves[u], split(between[u])) for u in units}
        size *= 2
    inverse = {u: split(inverse[u]) for u in units}

    solved = [[] for _ in range(group_size)]
    for s in range(len(half)):
        for n in range(group_size):
            write = writes[n][half[s]]
            key_part = (write * jnp.exp(log_cols[n][half[s]]) * key_scale[half[s]]) * key_f[half[s]]
            value_part = write * v_ref[half[s], n * width : (n + 1) * width].astype(f32)
            right = jnp.concatenate([key_part, value_part], axis=1)
            if s:
                done = split(jnp.concatenate(solved[n], axis=0))
                right = right - mm3(split(systems[n][half[s], : s * HALF]), done)
            solved[n].append(mm3(inverse[n, s], split(right)))

    eye = jnp.where(r == c, 1.0, 0.0)
    for n in range(group_size):
        full = split(jnp.concatenate(solved[n], axis=0))
        log_col = log_cols[n]
        mixed = mm3(split(mixings[n]), full)
        reach = (jnp.exp(log_col) * query_scale) * query_f - mixed[:, :width]
        reach_ref[n] = reach
        near_ref[n] = mixed[:, width:]
        last = log_col[length - 1 :]
        trailing = split((jnp.exp(last - log_col) * key_scale) * key_f)
        maps = mm3(trailing, full, TN)
        transit_ref[n] = jnp.exp(last) * eye - maps[:, :width]
        offset_ref[n] = maps[:, width:]


def local_phase(queries, key_vecs, values, strength, decay_rate, interpret=False):
    length, heads_k, width = queries.shape
    heads_v = values.shape[1]
    group_size = heads_v // heads_k
    per_head = lambda rows: pl.BlockSpec((group_size, rows, width), lambda i: (i, 0, 0))
    lanes = lambda n: pl.BlockSpec((length, n * width), lambda i: (0, i))
    whole = pl.BlockSpec((length, heads_v), lambda i: (0, 0))
    return pl.pallas_call(
        functools.partial(local_kernel, group_size),
        grid=(heads_k,),
        in_specs=[lanes(1), lanes(1), lanes(group_size), whole, whole],
        out_specs=[per_head(width), per_head(width), per_head(length), per_head(length)],
        out_shape=[
            jax.ShapeDtypeStruct((heads_v, width, width), f32),
            jax.ShapeDtypeStruct((heads_v, width, width), f32),
            jax.ShapeDtypeStruct((heads_v, length, width), f32),
            jax.ShapeDtypeStruct((heads_v, length, width), f32),
        ],
        interpret=interpret,
        name="local_phase",
    )(
        queries.reshape(length, heads_k * width),
        key_vecs.reshape(length, heads_k * width),
        values.reshape(length, heads_v * width),
        strength,
        decay_rate,
    )


MESH = pl.DeviceIdType.MESH
PIECES = 4


def finish_kernel(
    np_seq,
    np_heads,
    transit_ref,
    offset_ref,
    reach_ref,
    near_ref,
    gain_ref,
    w_hbm,
    out_ref,
    w_ref,
    state_ref,
    next_ref,
    normed_ref,
    part_ref,
    right_ref,
    left_ref,
    w_sem,
    state_send,
    state_recv,
    right_send,
    right_recv,
    left_send,
    left_recv,
):
    p, m = lax.axis_index("seq"), lax.axis_index("heads")
    heads, length, width = near_ref.shape
    rows = length // np_heads
    columns = out_ref.shape[1]
    piece = columns // PIECES

    load = pltpu.make_async_copy(w_hbm, w_ref, w_sem)
    load.start()

    barrier = pltpu.get_barrier_semaphore()
    neighbours = (
        {"seq": lax.rem(p + 1, np_seq)},
        {"seq": lax.rem(p + np_seq - 1, np_seq)},
        {"heads": lax.rem(m + 1, np_heads)},
        {"heads": lax.rem(m + np_heads - 1, np_heads)},
    )
    for where in neighbours:
        pl.semaphore_signal(barrier, inc=1, device_id=where, device_id_type=MESH)
    pl.semaphore_wait(barrier, len(neighbours))

    def hop(h):
        return pltpu.make_async_remote_copy(
            src_ref=next_ref.at[h],
            dst_ref=state_ref.at[h],
            send_sem=state_send.at[h],
            recv_sem=state_recv.at[h],
            device_id={"seq": p + 1},
            device_id_type=MESH,
        )

    @pl.when(p == 0)
    def _():
        state_ref[...] = jnp.zeros_like(state_ref)

    @pl.loop(0, heads)
    def _(h):
        transit = split(transit_ref[h])

        @pl.when(p > 0)
        def _():
            hop(h).wait_recv()

        @pl.when(p < np_seq - 1)
        def _():
            next_ref[h] = mm3(transit, split(state_ref[h])) + offset_ref[h]
            hop(h).start()

    for h in range(heads):
        core = near_ref[h] + mm3(split(reach_ref[h]), split(state_ref[h]))
        mean_sq = jnp.mean(core * core, axis=1, keepdims=True)
        normed = core * lax.rsqrt(mean_sq + norm_eps) * gain_ref[...]
        normed_ref[:, h * width : (h + 1) * width] = normed.astype(bf16)
    load.wait()

    def flow(buffer, send, recv, d, c, target):
        return pltpu.make_async_remote_copy(
            src_ref=part_ref.at[d, c],
            dst_ref=buffer.at[d, c],
            send_sem=send.at[d, c],
            recv_sem=recv.at[d, c],
            device_id={"heads": target},
            device_id_type=MESH,
        )

    right = lambda d, c: flow(right_ref, right_send, right_recv, d, c, m + 1)
    left = lambda d, c: flow(left_ref, left_send, left_recv, d, c, m - 1)

    def pass_on(d, c):
        if d > 0:

            @pl.when(m < d)
            def _():
                @pl.when(m > 0)
                def _():
                    right(d, c).wait_recv()
                    part_ref[d, c] += right_ref[d, c]

                right(d, c).start()

        if d < np_heads - 1:

            @pl.when(m > d)
            def _():
                @pl.when(m < np_heads - 1)
                def _():
                    left(d, c).wait_recv()
                    part_ref[d, c] += left_ref[d, c]

                left(d, c).start()

    order = []
    for i in range(np_heads):
        group = [d for d in dict.fromkeys((np_heads - 1 - i, i)) if d not in sum(order, [])]
        if group:
            order.append(group)
    for group in order:
        for c in range(PIECES):
            for d in group:
                part_ref[d, c] = mm(
                    normed_ref[d * rows : (d + 1) * rows, :],
                    w_ref[:, c * piece : (c + 1) * piece],
                )
        for c in range(PIECES):
            for d in group:
                pass_on(d, c)

    for c in range(PIECES):

        @pl.when(m > 0)
        def _():
            right(m, c).wait_recv()
            part_ref[m, c] += right_ref[m, c]

        @pl.when(m < np_heads - 1)
        def _():
            left(m, c).wait_recv()
            part_ref[m, c] += left_ref[m, c]

        out_ref[:, c * piece : (c + 1) * piece] = part_ref[m, c].astype(bf16)

    @pl.when(p < np_seq - 1)
    def _():
        for h in range(heads):
            hop(h).wait_send()

    for d in range(np_heads):
        for c in range(PIECES):
            if d > 0:

                @pl.when(m < d)
                def _():
                    right(d, c).wait_send()

            if d < np_heads - 1:

                @pl.when(m > d)
                def _():
                    left(d, c).wait_send()


def finish(np_seq, np_heads, transit, offset, reach, near, norm_gain, w_out):
    heads, length, width = near.shape
    columns = w_out.shape[1]
    rows = length // np_heads
    vmem = pl.BlockSpec(memory_space=pltpu.VMEM)
    slots = (np_heads, PIECES)
    dma = pltpu.SemaphoreType.DMA
    return pl.pallas_call(
        functools.partial(finish_kernel, np_seq, np_heads),
        out_shape=jax.ShapeDtypeStruct((rows, columns), bf16),
        in_specs=[vmem] * 5 + [pl.BlockSpec(memory_space=pl.ANY)],
        out_specs=vmem,
        scratch_shapes=[
            pltpu.VMEM(w_out.shape, bf16),
            pltpu.VMEM((heads, width, width), f32),
            pltpu.VMEM((heads, width, width), f32),
            pltpu.VMEM((length, heads * width), bf16),
        ]
        + [pltpu.VMEM(slots + (rows, columns // PIECES), f32)] * 3
        + [dma, dma((heads,)), dma((heads,)), dma(slots), dma(slots), dma(slots), dma(slots)],
        compiler_params=pltpu.CompilerParams(collective_id=0, has_side_effects=True),
        name="finish",
    )(transit, offset, reach, near, norm_gain.reshape(1, width), w_out)


def body(np_seq, np_heads, queries, key_vecs, values, strength, decay_rate, norm_gain, w_out):
    maps = local_phase(queries, key_vecs, values, strength, decay_rate)
    return finish(np_seq, np_heads, *maps, norm_gain, w_out)


def solution(mesh):
    return jax.shard_map(
        functools.partial(body, mesh.shape["seq"], mesh.shape["heads"]),
        mesh=mesh,
        in_specs=(
            P("seq", "heads", None),
            P("seq", "heads", None),
            P("seq", "heads", None),
            P("seq", "heads"),
            P("seq", "heads"),
            P(),
            P("heads", None),
        ),
        out_specs=P(("seq", "heads"), None),
        check_vma=False,
    )
```

```python
import functools

import jax
import jax.numpy as jnp
from jax import lax
from jax.experimental import pallas as pl
from jax.experimental.pallas import tpu as pltpu
from jax.sharding import PartitionSpec as P

norm_eps = 1e-12
unit_eps = 1e-06
BASE = 16
HALF = 128
f32, bf16 = jnp.float32, jnp.bfloat16

NN = (((1,), (0,)), ((), ()))
NT = (((1,), (1,)), ((), ()))
TN = (((0,), (0,)), ((), ()))


def mm(a, b, dims=NN):
    return lax.dot_general(a, b, dims, preferred_element_type=f32)


def split(x):
    high = x.astype(bf16)
    return high, (x - high.astype(f32)).astype(bf16)


def split3(x):
    high = x.astype(bf16)
    rest = x - high.astype(f32)
    mid = rest.astype(bf16)
    return high, mid, (rest - mid.astype(f32)).astype(bf16)


def mm3(a, b, dims=NN):
    return mm(a[0], b[0], dims) + (mm(a[0], b[1], dims) + mm(a[1], b[0], dims))


def iota(shape, dim):
    return lax.broadcasted_iota(jnp.int32, shape, dim)


def diagonal_inverses(systems, length):
    count = length // BASE
    lane = iota((BASE, length), 1)
    packed = []
    for low in systems:
        rows = jnp.zeros((BASE, length), f32)
        for b in range(count):
            rows = rows + jnp.where(lane // BASE == b, low[b * BASE : (b + 1) * BASE], 0.0)
        packed.append(rows)
    packed = jnp.concatenate(packed, axis=0)
    total = packed.shape[0]
    parts = []
    for start in range(0, length, 128):
        chunk = packed[:, start : start + 128]
        group = iota((total, 128), 1) // BASE * BASE
        local = iota((total, 128), 1) % BASE
        parts.append((chunk, group))
    outs = []
    for chunk, group in parts:
        solved = [
            jnp.where(iota((BASE, 128), 0) == iota((BASE, 128), 1) % BASE, 1.0, 0.0).astype(f32)
            for _ in systems
        ]
        for j in range(BASE - 1):
            column = jnp.take_along_axis(chunk, group + j, axis=1)
            solved = [
                x - column[n * BASE : (n + 1) * BASE] * x[j : j + 1] for n, x in enumerate(solved)
            ]
        outs.append(solved)
    return [[outs[c][n] for c in range(len(outs))] for n in range(len(systems))]


def spread(block):
    lane = iota((BASE, HALF), 1)
    return jnp.concatenate(
        [jnp.where(lane // BASE == b, block, 0.0) for b in range(HALF // BASE)], axis=0
    )


def local_kernel(
    group_size, q_ref, k_ref, v_ref, strength_ref, decay_ref, transit_ref, offset_ref, reach_ref, near_ref
):
    step = pl.program_id(0)
    length = q_ref.shape[0]
    heads = decay_ref.shape[0]
    width = k_ref.shape[1]
    query, key = q_ref[...], k_ref[...]
    query_f, key_f = query.astype(f32), key.astype(f32)
    query_scale = lax.rsqrt(jnp.sum(query_f * query_f, axis=1, keepdims=True) + unit_eps)
    key_sq = key_f * key_f
    key_scale = lax.rsqrt(jnp.sum(key_sq, axis=1, keepdims=True) + unit_eps)
    ones = jnp.ones((8, width), bf16)
    sq_high, sq_low = split(key_sq)
    key_scale_row = lax.rsqrt(mm(ones, sq_high, NT)[:1] + mm(ones, sq_low, NT)[:1] + unit_eps)

    row, col = iota((length, length), 0), iota((length, length), 1)
    lower = jnp.where(row >= col, 1.0, 0.0).astype(bf16)
    upper = jnp.where(row <= col, 1.0, 0.0).astype(bf16)
    pieces = split3(-decay_ref[...])
    logs = mm(lower, pieces[0], NT) + (mm(lower, pieces[1], NT) + mm(lower, pieces[2], NT))
    logs_row = mm(pieces[0], upper) + (mm(pieces[1], upper) + mm(pieces[2], upper))
    same = jnp.where(row == col, 1.0, 0.0).astype(bf16)
    strong = split3(strength_ref[...])
    strengths = mm(same, strong[0], NT) + (mm(same, strong[1], NT) + mm(same, strong[2], NT))

    key_dots = mm(key, key, NT) * key_scale * key_scale_row
    query_dots = mm(query, key, NT) * query_scale * key_scale_row

    half = [slice(s, s + HALF) for s in range(0, length, HALF)]
    systems, mixings, log_cols, writes = [], [], [], []
    for n in range(group_size):
        head = step * group_size + n
        lane = iota((length, heads), 1)
        log_col = jnp.sum(jnp.where(lane == head, logs, 0.0), axis=1, keepdims=True)
        write = jnp.sum(jnp.where(lane == head, strengths, 0.0), axis=1, keepdims=True)
        log_row = jnp.sum(
            jnp.where(iota((heads, length), 0) == head, logs_row, 0.0), axis=0, keepdims=True
        )
        ratio = jnp.exp(jnp.minimum(log_col - log_row, 0.0))
        systems.append(jnp.where(row > col, write * ratio * key_dots, 0.0))
        mixings.append(jnp.where(row >= col, ratio * query_dots, 0.0))
        log_cols.append(log_col)
        writes.append(write)

    base = diagonal_inverses(systems, length)
    r, c = iota((HALF, HALF), 0), iota((HALF, HALF), 1)
    units = [(n, s) for n in range(group_size) for s in range(len(half))]
    inverse = {u: spread(base[u[0]][u[1]]) for u in units}
    size = BASE
    while size < HALF:
        joint = (r // (2 * size) == c // (2 * size)) & (r // size > c // size)
        halves = {u: split(inverse[u]) for u in units}
        between = {
            u: mm3(split(jnp.where(joint, systems[u[0]][half[u[1]], half[u[1]]], 0.0)), halves[u])
            for u in units
        }
        inverse = {u: inverse[u] - mm3(halves[u], split(between[u])) for u in units}
        size *= 2
    inverse = {u: split(inverse[u]) for u in units}

    solved = [[] for _ in range(group_size)]
    for s in range(len(half)):
        for n in range(group_size):
            write = writes[n][half[s]]
            key_part = (write * jnp.exp(log_cols[n][half[s]]) * key_scale[half[s]]) * key_f[half[s]]
            value_part = write * v_ref[half[s], n * width : (n + 1) * width].astype(f32)
            right = jnp.concatenate([key_part, value_part], axis=1)
            if s:
                done = split(jnp.concatenate(solved[n], axis=0))
                right = right - mm3(split(systems[n][half[s], : s * HALF]), done)
            solved[n].append(mm3(inverse[n, s], split(right)))

    eye = jnp.where(r == c, 1.0, 0.0)
    for n in range(group_size):
        full = split(jnp.concatenate(solved[n], axis=0))
        log_col = log_cols[n]
        mixed = mm3(split(mixings[n]), full)
        reach = (jnp.exp(log_col) * query_scale) * query_f - mixed[:, :width]
        reach_ref[n] = reach
        near_ref[n] = mixed[:, width:]
        last = log_col[length - 1 :]
        trailing = split((jnp.exp(last - log_col) * key_scale) * key_f)
        maps = mm3(trailing, full, TN)
        transit_ref[n] = jnp.exp(last) * eye - maps[:, :width]
        offset_ref[n] = maps[:, width:]


def local_phase(queries, key_vecs, values, strength, decay_rate, interpret=False):
    length, heads_k, width = queries.shape
    heads_v = values.shape[1]
    group_size = heads_v // heads_k
    per_head = lambda rows: pl.BlockSpec((group_size, rows, width), lambda i: (i, 0, 0))
    lanes = lambda n: pl.BlockSpec((length, n * width), lambda i: (0, i))
    whole = pl.BlockSpec((heads_v, length), lambda i: (0, 0))
    return pl.pallas_call(
        functools.partial(local_kernel, group_size),
        grid=(heads_k,),
        in_specs=[lanes(1), lanes(1), lanes(group_size), whole, whole],
        out_specs=[per_head(width), per_head(width), per_head(length), per_head(length)],
        out_shape=[
            jax.ShapeDtypeStruct((heads_v, width, width), f32),
            jax.ShapeDtypeStruct((heads_v, width, width), f32),
            jax.ShapeDtypeStruct((heads_v, length, width), f32),
            jax.ShapeDtypeStruct((heads_v, length, width), f32),
        ],
        interpret=interpret,
        name="local_phase",
    )(
        queries.reshape(length, heads_k * width),
        key_vecs.reshape(length, heads_k * width),
        values.reshape(length, heads_v * width),
        jnp.transpose(strength),
        jnp.transpose(decay_rate),
    )


MESH = pl.DeviceIdType.MESH
PIECES = 8


def finish_kernel(
    np_seq,
    np_heads,
    transit_ref,
    offset_ref,
    reach_ref,
    near_ref,
    gain_ref,
    w_hbm,
    out_ref,
    w_ref,
    state_ref,
    next_ref,
    normed_ref,
    part_ref,
    right_ref,
    left_ref,
    w_sem,
    state_send,
    state_recv,
    right_send,
    right_recv,
    left_send,
    left_recv,
):
    p, m = lax.axis_index("seq"), lax.axis_index("heads")
    heads, length, width = near_ref.shape
    rows = length // np_heads
    columns = out_ref.shape[1]
    piece = columns // PIECES

    load = pltpu.make_async_copy(w_hbm, w_ref, w_sem)
    load.start()

    barrier = pltpu.get_barrier_semaphore()
    neighbours = (
        {"seq": lax.rem(p + 1, np_seq)},
        {"seq": lax.rem(p + np_seq - 1, np_seq)},
        {"heads": lax.rem(m + 1, np_heads)},
        {"heads": lax.rem(m + np_heads - 1, np_heads)},
    )
    for where in neighbours:
        pl.semaphore_signal(barrier, inc=1, device_id=where, device_id_type=MESH)
    pl.semaphore_wait(barrier, len(neighbours))

    def hop(h):
        return pltpu.make_async_remote_copy(
            src_ref=next_ref.at[h],
            dst_ref=state_ref.at[h],
            send_sem=state_send.at[h],
            recv_sem=state_recv.at[h],
            device_id={"seq": p + 1},
            device_id_type=MESH,
        )

    @pl.when(p == 0)
    def _():
        state_ref[...] = jnp.zeros_like(state_ref)

    @pl.loop(0, heads)
    def _(h):
        transit = split(transit_ref[h])

        @pl.when(p > 0)
        def _():
            hop(h).wait_recv()

        @pl.when(p < np_seq - 1)
        def _():
            next_ref[h] = mm3(transit, split(state_ref[h])) + offset_ref[h]
            hop(h).start()

    for h in range(heads):
        core = near_ref[h] + mm3(split(reach_ref[h]), split(state_ref[h]))
        mean_sq = jnp.mean(core * core, axis=1, keepdims=True)
        normed = core * lax.rsqrt(mean_sq + norm_eps) * gain_ref[...]
        normed_ref[:, h * width : (h + 1) * width] = normed.astype(bf16)
    load.wait()

    def flow(buffer, send, recv, d, c, target):
        return pltpu.make_async_remote_copy(
            src_ref=part_ref.at[d, c],
            dst_ref=buffer.at[d, c],
            send_sem=send.at[d, c],
            recv_sem=recv.at[d, c],
            device_id={"heads": target},
            device_id_type=MESH,
        )

    right = lambda d, c: flow(right_ref, right_send, right_recv, d, c, m + 1)
    left = lambda d, c: flow(left_ref, left_send, left_recv, d, c, m - 1)

    def pass_right(d, c):
        @pl.when(m < d)
        def _():
            @pl.when(m > 0)
            def _():
                right(d, c).wait_recv()
                part_ref[d, c] += right_ref[d, c]

            right(d, c).start()

    def pass_left(d, c):
        @pl.when(m > d)
        def _():
            @pl.when(m < np_heads - 1)
            def _():
                left(d, c).wait_recv()
                part_ref[d, c] += left_ref[d, c]

            left(d, c).start()

    ready = []
    for i in range(np_heads):
        far = np_heads - 1 - i
        for d in (far, i):
            if d not in ready:
                ready.append(d)
                for c in range(PIECES):
                    part_ref[d, c] = mm(
                        normed_ref[d * rows : (d + 1) * rows, :],
                        w_ref[:, c * piece : (c + 1) * piece],
                    )
        if far:
            for c in range(PIECES):
                pass_right(far, c)
                pass_left(i, c)

    for c in range(PIECES):

        @pl.when(m > 0)
        def _():
            right(m, c).wait_recv()
            part_ref[m, c] += right_ref[m, c]

        @pl.when(m < np_heads - 1)
        def _():
            left(m, c).wait_recv()
            part_ref[m, c] += left_ref[m, c]

        out_ref[:, c * piece : (c + 1) * piece] = part_ref[m, c].astype(bf16)

    @pl.when(p < np_seq - 1)
    def _():
        for h in range(heads):
            hop(h).wait_send()

    for d in range(np_heads):
        for c in range(PIECES):
            if d > 0:

                @pl.when(m < d)
                def _():
                    right(d, c).wait_send()

            if d < np_heads - 1:

                @pl.when(m > d)
                def _():
                    left(d, c).wait_send()


def finish(np_seq, np_heads, transit, offset, reach, near, norm_gain, w_out):
    heads, length, width = near.shape
    columns = w_out.shape[1]
    rows = length // np_heads
    vmem = pl.BlockSpec(memory_space=pltpu.VMEM)
    slots = (np_heads, PIECES)
    dma = pltpu.SemaphoreType.DMA
    return pl.pallas_call(
        functools.partial(finish_kernel, np_seq, np_heads),
        out_shape=jax.ShapeDtypeStruct((rows, columns), bf16),
        in_specs=[vmem] * 5 + [pl.BlockSpec(memory_space=pl.ANY)],
        out_specs=vmem,
        scratch_shapes=[
            pltpu.VMEM(w_out.shape, bf16),
            pltpu.VMEM((heads, width, width), f32),
            pltpu.VMEM((heads, width, width), f32),
            pltpu.VMEM((length, heads * width), bf16),
        ]
        + [pltpu.VMEM(slots + (rows, columns // PIECES), f32)] * 3
        + [dma, dma((heads,)), dma((heads,)), dma(slots), dma(slots), dma(slots), dma(slots)],
        compiler_params=pltpu.CompilerParams(collective_id=0, has_side_effects=True),
        name="finish",
    )(transit, offset, reach, near, norm_gain.reshape(1, width), w_out)


def body(np_seq, np_heads, queries, key_vecs, values, strength, decay_rate, norm_gain, w_out):
    maps = local_phase(queries, key_vecs, values, strength, decay_rate)
    return finish(np_seq, np_heads, *maps, norm_gain, w_out)


def solution(mesh):
    return jax.shard_map(
        functools.partial(body, mesh.shape["seq"], mesh.shape["heads"]),
        mesh=mesh,
        in_specs=(
            P("seq", "heads", None),
            P("seq", "heads", None),
            P("seq", "heads", None),
            P("seq", "heads"),
            P("seq", "heads"),
            P(),
            P("heads", None),
        ),
        out_specs=P(("seq", "heads"), None),
        check_vma=False,
    )
```

```python
import functools

import jax
import jax.numpy as jnp
from jax import lax
from jax.experimental import pallas as pl
from jax.experimental.pallas import tpu as pltpu
from jax.sharding import PartitionSpec as P

norm_eps = 1e-12
unit_eps = 1e-06
BASE = 16
HALF = 128
f32, bf16 = jnp.float32, jnp.bfloat16

NN = (((1,), (0,)), ((), ()))
NT = (((1,), (1,)), ((), ()))
TN = (((0,), (0,)), ((), ()))


def mm(a, b, dims=NN):
    return lax.dot_general(a, b, dims, preferred_element_type=f32)


def split(x):
    high = x.astype(bf16)
    return high, (x - high.astype(f32)).astype(bf16)


def split3(x):
    high = x.astype(bf16)
    rest = x - high.astype(f32)
    mid = rest.astype(bf16)
    return high, mid, (rest - mid.astype(f32)).astype(bf16)


def mm3(a, b, dims=NN):
    return mm(a[0], b[0], dims) + (mm(a[0], b[1], dims) + mm(a[1], b[0], dims))


def iota(shape, dim):
    return lax.broadcasted_iota(jnp.int32, shape, dim)


def diagonal_inverses(systems, length):
    count = length // BASE
    lane = iota((BASE, length), 1)
    packed = []
    for low in systems:
        rows = jnp.zeros((BASE, length), f32)
        for b in range(count):
            rows = rows + jnp.where(lane // BASE == b, low[b * BASE : (b + 1) * BASE], 0.0)
        packed.append(rows)
    packed = jnp.concatenate(packed, axis=0)
    total = packed.shape[0]
    parts = []
    for start in range(0, length, 128):
        chunk = packed[:, start : start + 128]
        group = iota((total, 128), 1) // BASE * BASE
        local = iota((total, 128), 1) % BASE
        parts.append((chunk, group))
    outs = []
    for chunk, group in parts:
        solved = [
            jnp.where(iota((BASE, 128), 0) == iota((BASE, 128), 1) % BASE, 1.0, 0.0).astype(f32)
            for _ in systems
        ]
        for j in range(BASE - 1):
            column = jnp.take_along_axis(chunk, group + j, axis=1)
            solved = [
                x - column[n * BASE : (n + 1) * BASE] * x[j : j + 1] for n, x in enumerate(solved)
            ]
        outs.append(solved)
    return [[outs[c][n] for c in range(len(outs))] for n in range(len(systems))]


def spread(block):
    lane = iota((BASE, HALF), 1)
    return jnp.concatenate(
        [jnp.where(lane // BASE == b, block, 0.0) for b in range(HALF // BASE)], axis=0
    )


def local_kernel(
    group_size, q_ref, k_ref, v_ref, strength_ref, decay_ref, transit_ref, offset_ref, reach_ref, near_ref
):
    step = pl.program_id(0)
    length = q_ref.shape[0]
    heads = decay_ref.shape[0]
    width = k_ref.shape[1]
    query, key = q_ref[...], k_ref[...]
    query_f, key_f = query.astype(f32), key.astype(f32)
    query_scale = lax.rsqrt(jnp.sum(query_f * query_f, axis=1, keepdims=True) + unit_eps)
    key_sq = key_f * key_f
    key_scale = lax.rsqrt(jnp.sum(key_sq, axis=1, keepdims=True) + unit_eps)
    ones = jnp.ones((8, width), bf16)
    sq_high, sq_low = split(key_sq)
    key_scale_row = lax.rsqrt(mm(ones, sq_high, NT)[:1] + mm(ones, sq_low, NT)[:1] + unit_eps)

    row, col = iota((length, length), 0), iota((length, length), 1)
    lower = jnp.where(row >= col, 1.0, 0.0).astype(bf16)
    upper = jnp.where(row <= col, 1.0, 0.0).astype(bf16)
    pieces = split3(-decay_ref[...])
    logs = mm(lower, pieces[0], NT) + (mm(lower, pieces[1], NT) + mm(lower, pieces[2], NT))
    logs_row = mm(pieces[0], upper) + (mm(pieces[1], upper) + mm(pieces[2], upper))
    same = jnp.where(row == col, 1.0, 0.0).astype(bf16)
    strong = split3(strength_ref[...])
    strengths = mm(same, strong[0], NT) + (mm(same, strong[1], NT) + mm(same, strong[2], NT))

    key_dots = mm(key, key, NT) * key_scale * key_scale_row
    query_dots = mm(query, key, NT) * query_scale * key_scale_row

    half = [slice(s, s + HALF) for s in range(0, length, HALF)]
    systems, mixings, log_cols, writes = [], [], [], []
    for n in range(group_size):
        head = step * group_size + n
        lane = iota((length, heads), 1)
        log_col = jnp.sum(jnp.where(lane == head, logs, 0.0), axis=1, keepdims=True)
        write = jnp.sum(jnp.where(lane == head, strengths, 0.0), axis=1, keepdims=True)
        log_row = jnp.sum(
            jnp.where(iota((heads, length), 0) == head, logs_row, 0.0), axis=0, keepdims=True
        )
        ratio = jnp.exp(jnp.minimum(log_col - log_row, 0.0))
        systems.append(jnp.where(row > col, write * ratio * key_dots, 0.0))
        mixings.append(jnp.where(row >= col, ratio * query_dots, 0.0))
        log_cols.append(log_col)
        writes.append(write)

    base = diagonal_inverses(systems, length)
    r, c = iota((HALF, HALF), 0), iota((HALF, HALF), 1)
    units = [(n, s) for n in range(group_size) for s in range(len(half))]
    inverse = {u: spread(base[u[0]][u[1]]) for u in units}
    size = BASE
    while size < HALF:
        joint = (r // (2 * size) == c // (2 * size)) & (r // size > c // size)
        halves = {u: split(inverse[u]) for u in units}
        between = {
            u: mm3(split(jnp.where(joint, systems[u[0]][half[u[1]], half[u[1]]], 0.0)), halves[u])
            for u in units
        }
        inverse = {u: inverse[u] - mm3(halves[u], split(between[u])) for u in units}
        size *= 2
    inverse = {u: split(inverse[u]) for u in units}

    solved = [[] for _ in range(group_size)]
    for s in range(len(half)):
        for n in range(group_size):
            write = writes[n][half[s]]
            key_part = (write * jnp.exp(log_cols[n][half[s]]) * key_scale[half[s]]) * key_f[half[s]]
            value_part = write * v_ref[half[s], n * width : (n + 1) * width].astype(f32)
            right = jnp.concatenate([key_part, value_part], axis=1)
            if s:
                done = split(jnp.concatenate(solved[n], axis=0))
                right = right - mm3(split(systems[n][half[s], : s * HALF]), done)
            solved[n].append(mm3(inverse[n, s], split(right)))

    eye = jnp.where(r == c, 1.0, 0.0)
    for n in range(group_size):
        full = split(jnp.concatenate(solved[n], axis=0))
        log_col = log_cols[n]
        mixed = mm3(split(mixings[n]), full)
        reach = (jnp.exp(log_col) * query_scale) * query_f - mixed[:, :width]
        reach_ref[n] = reach
        near_ref[n] = mixed[:, width:]
        last = log_col[length - 1 :]
        trailing = split((jnp.exp(last - log_col) * key_scale) * key_f)
        maps = mm3(trailing, full, TN)
        transit_ref[n] = jnp.exp(last) * eye - maps[:, :width]
        offset_ref[n] = maps[:, width:]


def local_phase(queries, key_vecs, values, strength, decay_rate, interpret=False):
    length, heads_k, width = queries.shape
    heads_v = values.shape[1]
    group_size = heads_v // heads_k
    per_head = lambda rows: pl.BlockSpec((group_size, rows, width), lambda i: (i, 0, 0))
    lanes = lambda n: pl.BlockSpec((length, n * width), lambda i: (0, i))
    whole = pl.BlockSpec((heads_v, length), lambda i: (0, 0))
    return pl.pallas_call(
        functools.partial(local_kernel, group_size),
        grid=(heads_k,),
        in_specs=[lanes(1), lanes(1), lanes(group_size), whole, whole],
        out_specs=[per_head(width), per_head(width), per_head(length), per_head(length)],
        out_shape=[
            jax.ShapeDtypeStruct((heads_v, width, width), f32),
            jax.ShapeDtypeStruct((heads_v, width, width), f32),
            jax.ShapeDtypeStruct((heads_v, length, width), f32),
            jax.ShapeDtypeStruct((heads_v, length, width), f32),
        ],
        interpret=interpret,
        name="local_phase",
    )(
        queries.reshape(length, heads_k * width),
        key_vecs.reshape(length, heads_k * width),
        values.reshape(length, heads_v * width),
        jnp.transpose(strength),
        jnp.transpose(decay_rate),
    )


MESH = pl.DeviceIdType.MESH
PIECES = 2


def finish_kernel(
    np_seq,
    np_heads,
    transit_ref,
    offset_ref,
    reach_ref,
    near_ref,
    gain_ref,
    w_hbm,
    out_ref,
    w_ref,
    state_ref,
    next_ref,
    normed_ref,
    part_ref,
    right_ref,
    left_ref,
    w_sem,
    state_send,
    state_recv,
    right_send,
    right_recv,
    left_send,
    left_recv,
):
    p, m = lax.axis_index("seq"), lax.axis_index("heads")
    heads, length, width = near_ref.shape
    rows = length // np_heads
    columns = out_ref.shape[1]
    piece = columns // PIECES

    load = pltpu.make_async_copy(w_hbm, w_ref, w_sem)
    load.start()

    barrier = pltpu.get_barrier_semaphore()
    neighbours = (
        {"seq": lax.rem(p + 1, np_seq)},
        {"seq": lax.rem(p + np_seq - 1, np_seq)},
        {"heads": lax.rem(m + 1, np_heads)},
        {"heads": lax.rem(m + np_heads - 1, np_heads)},
    )
    for where in neighbours:
        pl.semaphore_signal(barrier, inc=1, device_id=where, device_id_type=MESH)
    pl.semaphore_wait(barrier, len(neighbours))

    def hop(h):
        return pltpu.make_async_remote_copy(
            src_ref=next_ref.at[h],
            dst_ref=state_ref.at[h],
            send_sem=state_send.at[h],
            recv_sem=state_recv.at[h],
            device_id={"seq": p + 1},
            device_id_type=MESH,
        )

    @pl.when(p == 0)
    def _():
        state_ref[...] = jnp.zeros_like(state_ref)

    @pl.loop(0, heads)
    def _(h):
        transit = split(transit_ref[h])

        @pl.when(p > 0)
        def _():
            hop(h).wait_recv()

        @pl.when(p < np_seq - 1)
        def _():
            next_ref[h] = mm3(transit, split(state_ref[h])) + offset_ref[h]
            hop(h).start()

    for h in range(heads):
        core = near_ref[h] + mm3(split(reach_ref[h]), split(state_ref[h]))
        mean_sq = jnp.mean(core * core, axis=1, keepdims=True)
        normed = core * lax.rsqrt(mean_sq + norm_eps) * gain_ref[...]
        normed_ref[:, h * width : (h + 1) * width] = normed.astype(bf16)
    load.wait()

    def flow(buffer, send, recv, d, c, target):
        return pltpu.make_async_remote_copy(
            src_ref=part_ref.at[d, c],
            dst_ref=buffer.at[d, c],
            send_sem=send.at[d, c],
            recv_sem=recv.at[d, c],
            device_id={"heads": target},
            device_id_type=MESH,
        )

    right = lambda d, c: flow(right_ref, right_send, right_recv, d, c, m + 1)
    left = lambda d, c: flow(left_ref, left_send, left_recv, d, c, m - 1)

    def pass_right(d, c):
        @pl.when(m < d)
        def _():
            @pl.when(m > 0)
            def _():
                right(d, c).wait_recv()
                part_ref[d, c] += right_ref[d, c]

            right(d, c).start()

    def pass_left(d, c):
        @pl.when(m > d)
        def _():
            @pl.when(m < np_heads - 1)
            def _():
                left(d, c).wait_recv()
                part_ref[d, c] += left_ref[d, c]

            left(d, c).start()

    ready = []
    for i in range(np_heads):
        far = np_heads - 1 - i
        for d in (far, i):
            if d not in ready:
                ready.append(d)
                for c in range(PIECES):
                    part_ref[d, c] = mm(
                        normed_ref[d * rows : (d + 1) * rows, :],
                        w_ref[:, c * piece : (c + 1) * piece],
                    )
        if far:
            for c in range(PIECES):
                pass_right(far, c)
                pass_left(i, c)

    for c in range(PIECES):

        @pl.when(m > 0)
        def _():
            right(m, c).wait_recv()
            part_ref[m, c] += right_ref[m, c]

        @pl.when(m < np_heads - 1)
        def _():
            left(m, c).wait_recv()
            part_ref[m, c] += left_ref[m, c]

        out_ref[:, c * piece : (c + 1) * piece] = part_ref[m, c].astype(bf16)

    @pl.when(p < np_seq - 1)
    def _():
        for h in range(heads):
            hop(h).wait_send()

    for d in range(np_heads):
        for c in range(PIECES):
            if d > 0:

                @pl.when(m < d)
                def _():
                    right(d, c).wait_send()

            if d < np_heads - 1:

                @pl.when(m > d)
                def _():
                    left(d, c).wait_send()


def finish(np_seq, np_heads, transit, offset, reach, near, norm_gain, w_out):
    heads, length, width = near.shape
    columns = w_out.shape[1]
    rows = length // np_heads
    vmem = pl.BlockSpec(memory_space=pltpu.VMEM)
    slots = (np_heads, PIECES)
    dma = pltpu.SemaphoreType.DMA
    return pl.pallas_call(
        functools.partial(finish_kernel, np_seq, np_heads),
        out_shape=jax.ShapeDtypeStruct((rows, columns), bf16),
        in_specs=[vmem] * 5 + [pl.BlockSpec(memory_space=pl.ANY)],
        out_specs=vmem,
        scratch_shapes=[
            pltpu.VMEM(w_out.shape, bf16),
            pltpu.VMEM((heads, width, width), f32),
            pltpu.VMEM((heads, width, width), f32),
            pltpu.VMEM((length, heads * width), bf16),
        ]
        + [pltpu.VMEM(slots + (rows, columns // PIECES), f32)] * 3
        + [dma, dma((heads,)), dma((heads,)), dma(slots), dma(slots), dma(slots), dma(slots)],
        compiler_params=pltpu.CompilerParams(collective_id=0, has_side_effects=True),
        name="finish",
    )(transit, offset, reach, near, norm_gain.reshape(1, width), w_out)


def body(np_seq, np_heads, queries, key_vecs, values, strength, decay_rate, norm_gain, w_out):
    maps = local_phase(queries, key_vecs, values, strength, decay_rate)
    return finish(np_seq, np_heads, *maps, norm_gain, w_out)


def solution(mesh):
    return jax.shard_map(
        functools.partial(body, mesh.shape["seq"], mesh.shape["heads"]),
        mesh=mesh,
        in_specs=(
            P("seq", "heads", None),
            P("seq", "heads", None),
            P("seq", "heads", None),
            P("seq", "heads"),
            P("seq", "heads"),
            P(),
            P("heads", None),
        ),
        out_specs=P(("seq", "heads"), None),
        check_vma=False,
    )
```
